32 devices in a mesh: terms: 32 (over z, y, x, core).
Axes of the slice: x: 2, y: 2, z: 4, core: 2. Of those that a mesh axis runs over, the one named last changes fastest.
Arguments:
- psi: float32 [2, 256, 4, 4, 256], replicated
- left_env: bfloat16 [256, 256, 256], P('terms')
- phys_op: bfloat16 [256, 16, 16], P('terms')
- right_env: bfloat16 [256, 256, 256], P('terms')
Outputs:
- output 1: float32 [2, 7, 256, 4, 4, 256], P(None, None, 'terms')
- output 2: float32 [2, 6], replicated
- output 3: float32 [2, 6], replicated
All inputs are finite; a program needn't handle non-finite values.
Results may differ from the reference program's by a relative error of at most 0.0122832.
Values are sent between devices in bfloat16 or wider.
A program may use at most 1 GiB of HBM per device.

```python
import jax
import jax.numpy as jnp
from jax import lax

BOND_DIM = 256
PHYS_DIM = 4
ROOT_COUNT = 2
TERM_COUNT = 256
LANCZOS_STEPS = 6
PAIRS = PHYS_DIM * PHYS_DIM
N_ELEMS = BOND_DIM * PAIRS * BOND_DIM


def symmetric_terms(key, count, width):
    noise_key, shift_key = jax.random.split(key)
    raw = jax.random.normal(noise_key, (count, width, width), jnp.float32)
    noise = (raw + jnp.swapaxes(raw, 1, 2)) * (2.0 * width) ** -0.5
    shift = jax.random.normal(shift_key, (count,), jnp.float32)
    return noise + shift[:, None, None] * jnp.eye(width, dtype=jnp.float32)


def setup_inputs(seed: int = 0) -> dict:
    keys = jax.random.split(jax.random.key(seed), 4)
    psi = jax.random.normal(keys[0], (ROOT_COUNT, BOND_DIM, PHYS_DIM, PHYS_DIM, BOND_DIM), jnp.float32)
    left_env = symmetric_terms(keys[1], TERM_COUNT, BOND_DIM).astype(jnp.bfloat16)
    phys_op = (symmetric_terms(keys[2], TERM_COUNT, PAIRS) * TERM_COUNT ** -0.5).astype(jnp.bfloat16)
    right_env = symmetric_terms(keys[3], TERM_COUNT, BOND_DIM).astype(jnp.bfloat16)
    return {'psi': psi, 'left_env': left_env, 'phys_op': phys_op, 'right_env': right_env}


def reference(psi, left_env, phys_op, right_env):
    psi_mat = psi.reshape(ROOT_COUNT, BOND_DIM, PAIRS, BOND_DIM)
    norms = jnp.sqrt(jnp.sum(psi_mat * psi_mat, axis=(1, 2, 3)) / N_ELEMS)
    v_start = psi_mat / norms[:, None, None, None]

    def matvec(v_cur):
        flat_in = v_cur.astype(jnp.bfloat16).reshape(ROOT_COUNT * BOND_DIM * PAIRS, BOND_DIM)

        def add_term(acc, term):
            left_k, phys_k, right_k = term
            right_part = jnp.dot(flat_in, right_k.T, preferred_element_type=jnp.float32).astype(jnp.bfloat16)
            right_part = right_part.reshape(ROOT_COUNT, BOND_DIM, PAIRS, BOND_DIM)
            mid_part = jnp.einsum('qu,rcub->rcqb', phys_k.astype(jnp.float32), right_part.astype(jnp.float32)).astype(jnp.bfloat16)
            left_part = jnp.einsum('ac,rcqb->raqb', left_k.astype(jnp.float32), mid_part.astype(jnp.float32))
            return acc + left_part, None

        zero_acc = jnp.zeros((ROOT_COUNT, BOND_DIM, PAIRS, BOND_DIM), jnp.float32)
        total, _ = lax.scan(add_term, zero_acc, (left_env, phys_op, right_env))
        return total

    def lanczos_step(carry, unused):
        v_prev, v_cur, beta_prev = carry
        sigma = matvec(v_cur)
        alpha = jnp.sum(sigma * v_cur, axis=(1, 2, 3)) / N_ELEMS
        residual = sigma - alpha[:, None, None, None] * v_cur - beta_prev[:, None, None, None] * v_prev
        beta = jnp.sqrt(jnp.sum(residual * residual, axis=(1, 2, 3)) / N_ELEMS)
        v_next = residual / beta[:, None, None, None]
        return (v_cur, v_next, beta), (v_next, alpha, beta)

    start_carry = (jnp.zeros_like(v_start), v_start, jnp.zeros((ROOT_COUNT,), jnp.float32))
    _, (later, alphas, betas) = lax.scan(lanczos_step, start_carry, None, length=LANCZOS_STEPS)
    vectors = jnp.concatenate([v_start[None], later], axis=0)
    vectors = jnp.transpose(vectors, (1, 0, 2, 3, 4)).reshape(ROOT_COUNT, LANCZOS_STEPS + 1, BOND_DIM, PHYS_DIM, PHYS_DIM, BOND_DIM)
    return (vectors, alphas.T, betas.T)
```

```python
import functools

import jax
import jax.numpy as jnp
from jax import lax
from jax.experimental import pallas as pl
from jax.experimental.pallas import tpu as pltpu
from jax.sharding import PartitionSpec as P

STEPS = 6
BF = jnp.bfloat16
F32 = jnp.float32
MESH = pl.DeviceIdType.MESH
VM = pltpu.VMEM
N_ELEMS = 256 * 16 * 256


def rcopy(src, dst, ss, rs, dev):
    return pltpu.make_async_remote_copy(src_ref=src, dst_ref=dst, send_sem=ss, recv_sem=rs, device_id=(dev,), device_id_type=MESH)


def greet(devs):
    bar = pltpu.get_barrier_semaphore()
    for d in devs:
        pl.semaphore_signal(bar, inc=1, device_id=(d,), device_id_type=MESH)
    pl.semaphore_wait(bar, len(devs))


def setup_kernel(l_ref, r_ref, w_ref, la, ra, wa, ls, zs, xs, ys, rsl, rss, rrs, wss, wrs):
    me = lax.axis_index("terms")
    c = lax.rem(me, 2)
    s = me // 2
    z = me // 8
    xn, yn = me ^ 2, me ^ 4
    sx, sy = s ^ 1, s ^ 2
    peers = [lax.rem(me + 2 * d, 32) for d in range(1, 16)]
    greet(peers)

    def half(ref, src, h):
        return ref.at[src, pl.ds(4 * h, 4)]

    own = [pltpu.make_async_copy(l_ref, la.at[s], ls.at[0]),
           pltpu.make_async_copy(r_ref.at[:, pl.ds(32 * lax.rem(s, 8), 32)], ra.at[s], ls.at[1]),
           pltpu.make_async_copy(w_ref, wa.at[s], ls.at[2])]
    for o in own:
        o.start()
    sends = []

    def send_z(src, k, mine, up):
        cond = (z < 3) if up else (z > 0)
        dev = me + 8 if up else me - 8
        for h in range(2):
            ref = l_ref.at[pl.ds(4 * h, 4)] if mine else half(la, src, h)
            cp = rcopy(ref, half(la, src, h), zs.at[0 if up else 1, k, h], rsl.at[src, h], dev)
            yield cp, cond

    def run_z(src, k, mine, up, guard):
        for cp, cond in send_z(src, k, mine, up):
            cc = cond if guard is None else jnp.logical_and(cond, guard)
            pl.when(cc)(cp.start)
            sends.append((cp, cc))

    def run_xy(src, k, mine, guard):
        for h, dev, sem in ((0, xn, xs.at[k]), (1, yn, ys.at[k]), (0, yn, ys.at[4 + k]), (1, xn, xs.at[4 + k])):
            ref = l_ref.at[pl.ds(4 * h, 4)] if mine else half(la, src, h)
            cp = rcopy(ref, half(la, src, h), sem, rsl.at[src, h], dev)
            if guard is None:
                cp.start()
            else:
                pl.when(guard)(cp.start)
            sends.append((cp, guard))

    def wait_in(src, h, guard):
        cp = rcopy(half(la, src, h), half(la, src, h), xs.at[0], rsl.at[src, h], xn)
        if guard is None:
            cp.wait_recv()
        else:
            pl.when(guard)(cp.wait_recv)

    def forward(srcx, srcy, k, guard):
        for src, h, dev, sem in ((srcx, 0, yn, ys.at[8 + k]), (srcy, 1, xn, xs.at[8 + k])):
            wait_in(src, h, guard)
            cp = rcopy(half(la, src, h), half(la, src, h), sem, rsl.at[src, h], dev)
            if guard is None:
                cp.start()
            else:
                pl.when(guard)(cp.start)
            sends.append((cp, guard))

    run_z(s, 0, True, True, None)
    run_z(s, 0, True, False, None)
    run_xy(s, 0, True, None)
    for d in range(1, 16):
        dst = lax.rem(s + d, 16)
        rsem = lax.rem(16 - d, 16)
        dev = 2 * dst + c
        cp = rcopy(r_ref.at[:, pl.ds(32 * lax.rem(dst, 8), 32)], ra.at[s], rss.at[d], rrs.at[rsem], dev)
        cp.start()
        sends.append((cp, "r"))
        cp = rcopy(w_ref, wa.at[s], wss.at[d], wrs.at[rsem], dev)
        cp.start()
        sends.append((cp, "r"))
    forward(sx, sy, 0, None)
    slot = [(1, -1), (1, 1), (2, -1), (2, 1), (3, -1), (3, 1)]
    pend = []
    for n, (e, sign) in enumerate(slot):
        guard = (z >= e) if sign < 0 else (z <= 3 - e)
        src = jnp.clip(s + 4 * e * sign, 0, 15)
        for h in range(2):
            wait_in(src, h, guard)
        if e < 3:
            run_z(src, e, False, sign < 0, guard)
        pend.append((src, sign, e, guard))
        k = jnp.where(sign < 0, z - e, z + e - 1)
        k = 1 + jnp.clip(k, 0, 2)
        run_xy(src, k, False, guard)
        forward(src ^ 1, src ^ 2, k, guard)
    for n in range(4):
        base = lax.rem(s, 4) + 4 * n
        wait_in(base ^ 1, 1, None)
        wait_in(base ^ 2, 0, None)
        wait_in(base ^ 3, 0, None)
        wait_in(base ^ 3, 1, None)
    for cp, guard in sends:
        if guard is None:
            cp.wait_send()
        elif isinstance(guard, str):
            cp.wait_send()
            cp.wait_recv()
        else:
            pl.when(guard)(cp.wait_send)
    for o in own:
        o.wait()


def setup(l_loc, r_loc, w_loc):
    any_ = pl.BlockSpec(memory_space=pl.ANY)
    vm = pl.BlockSpec(memory_space=VM)
    dma = pltpu.SemaphoreType.DMA
    return pl.pallas_call(
        setup_kernel,
        out_shape=(jax.ShapeDtypeStruct((16, 8, 256, 256), BF), jax.ShapeDtypeStruct((16, 8, 32, 256), BF), jax.ShapeDtypeStruct((16, 16, 128), BF)),
        in_specs=[vm, vm, vm],
        out_specs=(any_, any_, any_),
        scratch_shapes=[dma((3,)), dma((2, 3, 2)), dma((12,)), dma((12,)), dma((16, 2)), dma((16,)), dma((16,)), dma((16,)), dma((16,))],
        compiler_params=pltpu.CompilerParams(collective_id=0, has_side_effects=True, vmem_limit_bytes=24 * 2**20),
    )(l_loc, r_loc, w_loc)


def kron_kernel(w_ref, o_ref):
    row = lax.broadcasted_iota(jnp.int32, (16, 256), 0)
    lane = lax.broadcasted_iota(jnp.int32, (16, 256), 1)
    mask = (lane & 15) == row
    for k in range(8):
        for q in range(16):
            v = jnp.broadcast_to(w_ref[k, q:q + 1, :], (16, 256))
            o_ref[k, q * 16:(q + 1) * 16, :] = jnp.where(mask, v, 0.0).astype(BF)


def kron(wexp):
    terms = wexp.shape[0]
    return pl.pallas_call(
        kron_kernel, grid=(terms // 8,),
        in_specs=[pl.BlockSpec((8, 16, 256), lambda i: (i, 0, 0))],
        out_specs=pl.BlockSpec((8, 256, 256), lambda i: (i, 0, 0)),
        out_shape=jax.ShapeDtypeStruct((terms, 256, 256), BF),
    )(wexp)


KC = 8


def matvec_kernel(u_ref, r_ref, w_ref, l_ref, o_ref, y, zz):
    @pl.when(pl.program_id(0) == 0)
    def _():
        o_ref[...] = jnp.zeros_like(o_ref)

    rb = r_ref[...].reshape(KC * 32, 256)
    for u in range(16):
        yu = jnp.dot(rb, u_ref[u], preferred_element_type=F32).astype(BF).reshape(KC, 2, 16, 256)
        for t in range(2):
            y[:, u * 16:(u + 1) * 16, t * 256:(t + 1) * 256] = yu[:, t]
    for k in range(KC):
        zk = jnp.dot(w_ref[k], y[k], preferred_element_type=F32).astype(BF)
        for t in range(2):
            zz[t * 256:(t + 1) * 256, k * 256:(k + 1) * 256] = zk[:, t * 256:(t + 1) * 256]
    o_ref[...] += jnp.dot(zz[...], l_ref[...].reshape(KC * 256, 256), preferred_element_type=F32)


def matvec(u, r, w, l):
    terms = l.shape[0]
    return pl.pallas_call(
        matvec_kernel, grid=(terms // KC,),
        in_specs=[pl.BlockSpec((16, 256, 256), lambda i: (0, 0, 0)), pl.BlockSpec((KC, 32, 256), lambda i: (i, 0, 0)),
                  pl.BlockSpec((KC, 256, 256), lambda i: (i, 0, 0)), pl.BlockSpec((KC, 256, 256), lambda i: (i, 0, 0))],
        out_specs=pl.BlockSpec((512, 256), lambda i: (0, 0)),
        out_shape=jax.ShapeDtypeStruct((512, 256), F32),
        scratch_shapes=[VM((KC, 256, 512), BF), VM((512, KC * 256), BF)],
        compiler_params=pltpu.CompilerParams(vmem_limit_bytes=40 * 2**20),
    )(u, r, w, l)


def update_kernel(last, part, v_ref, vp_ref, bp_ref, vn_ref, u_ref, ab_ref, got, sc_out, sc_in, ps, sss, srs, uss, urs, fss):
    me = lax.axis_index("terms")
    c = lax.rem(me, 2)
    half = me // 16
    m = lax.rem(me, 16)
    sib = me ^ 1
    others = [16 * half + (m ^ d) for d in range(1, 16)]
    greet(others)
    swap = rcopy(part.at[1 - c], got, ps.at[0], ps.at[1], sib)
    swap.start()
    swap.wait()
    v = v_ref[...]
    w = part[c] + got[...]
    w2 = w - bp_ref[1:2, 0:1] * vp_ref[...]
    s1 = jnp.sum(w * v)
    s4 = jnp.sum(v * v)
    sh = jnp.sum(w2 * v) / jnp.where(s4 > 0, s4, 1.0)
    w3 = w2 - sh * v
    s2 = jnp.sum(w3 * w3)
    s3 = jnp.sum(w3 * v)
    row = lax.broadcasted_iota(jnp.int32, (8, 128), 0)
    tile = jnp.zeros((8, 128), F32)
    for n, val in enumerate((s1, s2, s3, s4, sh)):
        tile = jnp.where(row == n, val, tile)
    sc_out[...] = tile
    sc_in[m] = tile
    sends = []
    for d in range(1, 16):
        cp = rcopy(sc_out, sc_in.at[m], sss.at[d], srs.at[d], others[d - 1])
        cp.start()
        sends.append(cp)
    for cp in sends:
        cp.wait()
    alpha = jnp.zeros((1, 1), F32)
    for d in range(16):
        alpha = alpha + sc_in[d, 0:1, 0:1]
    alpha = alpha / N_ELEMS
    beta2 = jnp.zeros((1, 1), F32)
    for d in range(16):
        dl = alpha - sc_in[d, 4:5, 0:1]
        beta2 = beta2 + (sc_in[d, 1:2, 0:1] - 2.0 * dl * sc_in[d, 2:3, 0:1] + dl * dl * sc_in[d, 3:4, 0:1])
    beta = jnp.sqrt(jnp.maximum(beta2, 0.0) / N_ELEMS)
    ab_ref[...] = jnp.where(row == 0, jnp.broadcast_to(alpha, (8, 128)), jnp.broadcast_to(beta, (8, 128)))
    vn = (w2 - alpha * v) / beta
    b0 = 16 * m

    def mine(src):
        return u_ref.at[:, pl.ds(16 * src, 16), :]

    if not last:
        u_ref[:, pl.ds(b0, 16), :] = vn.astype(BF).reshape(16, 16, 256)
    vn_ref[...] = vn
    if not last:
        sends = []
        for d in range(1, 16):
            if d == 1 or d % 2 == 0:
                cp = rcopy(mine(m), mine(m), uss.at[d], urs.at[d], others[d - 1])
                cp.start()
                sends.append((d, cp))
        for d, cp in sends[1:]:
            cp.wait_recv()
            fw = rcopy(mine(m ^ d), mine(m ^ d), fss.at[d], urs.at[d + 1], sib)
            fw.start()
            sends.append((d + 1, fw))
        sends[0][1].wait_recv()
        for d, cp in sends[8:]:
            cp.wait_recv()
        for d, cp in sends:
            cp.wait_send()


def update(part, v, vp, bp, last):
    vm = pl.BlockSpec(memory_space=VM)
    dma = pltpu.SemaphoreType.DMA
    return pl.pallas_call(
        functools.partial(update_kernel, last),
        out_shape=(jax.ShapeDtypeStruct((256, 256), F32), jax.ShapeDtypeStruct((16, 256, 256), BF), jax.ShapeDtypeStruct((8, 128), F32)),
        in_specs=[vm] * 4,
        out_specs=(vm, vm, vm),
        scratch_shapes=[VM((256, 256), F32), VM((8, 128), F32), VM((16, 8, 128), F32), dma((2,)), dma((16,)), dma((16,)), dma((16,)), dma((16,)), dma((16,))],
        compiler_params=pltpu.CompilerParams(collective_id=2 if last else 1, has_side_effects=True, vmem_limit_bytes=24 * 2**20),
    )(part.reshape(2, 256, 256), v, vp, bp)


def finish_kernel(v0_ref, *refs):
    vs = refs[:STEPS]
    abs_ = refs[STEPS:2 * STEPS]
    o_ref, ab_ref, tb, rx, ss, rs, xs = refs[2 * STEPS:]
    me = lax.axis_index("terms")
    half = me // 16
    row = lax.broadcasted_iota(jnp.int32, (8, 128), 0)
    lane = lax.broadcasted_iota(jnp.int32, (8, 128), 1)
    tile = jnp.zeros((8, 128), F32)
    for j in range(STEPS):
        tb[j] = vs[j][...].T
        tile = jnp.where(lane == j, abs_[j][...], tile)
    ab_ref[half] = tile
    greet([me ^ d for d in range(1, 32)])
    sends = []
    cross = rcopy(ab_ref.at[half], ab_ref.at[half], xs.at[0], xs.at[1], me ^ 16)
    cross.start()
    for d in range(31, 0, -1):
        p = me ^ d
        cp = rcopy(tb.at[:, pl.ds(pl.multiple_of(8 * p, 8), 8), :], rx.at[me], ss.at[d], rs.at[d], p)
        cp.start()
        sends.append(cp)
    for r in range(2):
        o_ref[r, 0] = v0_ref[r]
    rx[me] = tb[:, pl.ds(pl.multiple_of(8 * me, 8), 8), :]
    for cp in sends:
        cp.wait()
    cross.wait()
    grp = lax.broadcasted_iota(jnp.int32, (8, 128), 1) // 16

    def body(n, carry):
        r = n // STEPS
        j = lax.rem(n, STEPS)
        for h in range(2):
            for hb in range(2):
                xv = [rx[16 * r + 8 * hb + q, j, :, h * 128:(h + 1) * 128] for q in range(8)]
                for d in (1, 2, 4):
                    low = (grp & d) == 0
                    for a in range(8):
                        if a & d == 0:
                            p, q = xv[a], xv[a + d]
                            xv[a] = jnp.where(low, p, pltpu.roll(q, 16 * d, 1))
                            xv[a + d] = jnp.where(low, pltpu.roll(p, 128 - 16 * d, 1), q)
                for q in range(8):
                    o_ref[r, j + 1, :, h * 8 + q, hb * 128:(hb + 1) * 128] = xv[q]
        return carry

    lax.fori_loop(0, 2 * STEPS, body, 0)


def finish(v0rows, vs, abs_):
    vm = pl.BlockSpec(memory_space=VM)
    dma = pltpu.SemaphoreType.DMA
    return pl.pallas_call(
        finish_kernel,
        out_shape=(jax.ShapeDtypeStruct((2, STEPS + 1, 8, 16, 256), F32), jax.ShapeDtypeStruct((2, 8, 128), F32)),
        in_specs=[vm] * (1 + 2 * STEPS),
        out_specs=(vm, vm),
        scratch_shapes=[VM((STEPS, 256, 256), F32), VM((32, STEPS, 8, 256), F32), dma((32,)), dma((32,)), dma((2,))],
        compiler_params=pltpu.CompilerParams(collective_id=3, has_side_effects=True, vmem_limit_bytes=40 * 2**20),
    )(v0rows, *vs, *abs_)


def solution(mesh):
    def device_fn(psi, l_loc, w_loc, r_loc):
        me = lax.axis_index("terms")
        half = me // 16
        m = lax.rem(me, 16)
        la, ra, wa = setup(l_loc, r_loc, w_loc.reshape(16, 128))
        la = la.reshape(128, 256, 256)
        ra = ra.reshape(128, 32, 256)
        wk = kron(jnp.repeat(wa.reshape(128, 16, 16).astype(F32), 16, axis=-1))
        psi = psi.reshape(2, 256, 16, 256)
        norms = jnp.sqrt(jnp.sum(psi * psi, axis=(1, 2, 3)) / N_ELEMS)
        v0rows = lax.dynamic_slice_in_dim(psi, 8 * me, 8, axis=1) / norms[:, None, None, None]
        mine = lax.dynamic_index_in_dim(psi, half, 0, keepdims=False)
        norm = lax.dynamic_index_in_dim(norms, half, 0, keepdims=False)
        u = (mine / norm).astype(BF).transpose(1, 2, 0)
        v = (lax.dynamic_slice_in_dim(mine, 16 * m, 16, axis=2) / norm).transpose(1, 2, 0).reshape(256, 256)
        vp = jnp.zeros_like(v)
        ab = jnp.zeros((8, 128), F32)
        vs, abs_ = [], []
        for j in range(STEPS):
            part = matvec(u, ra, wk, la)
            vn, u, ab = update(part, v, vp, ab, j == STEPS - 1)
            vs.append(vn)
            abs_.append(ab)
            vp, v = v, vn
        vecs, abo = finish(v0rows, vs, abs_)
        return vecs.reshape(2, STEPS + 1, 8, 4, 4, 256), abo[:, 0, :STEPS], abo[:, 1, :STEPS]

    return jax.shard_map(device_fn, mesh=mesh, in_specs=(P(), P("terms"), P("terms"), P("terms")),
                         out_specs=(P(None, None, "terms"), P(), P()), check_vma=False)
```

```python
import functools

import jax
import jax.numpy as jnp
from jax import lax
from jax.experimental import pallas as pl
from jax.experimental.pallas import tpu as pltpu
from jax.sharding import PartitionSpec as P

STEPS = 6
KC = 8
BF = jnp.bfloat16
F32 = jnp.float32
MESH = pl.DeviceIdType.MESH
VM = pltpu.VMEM
D, H = 256, 128
N_ELEMS = D * 16 * D
TILE = (8, H)
NEAR = (2, 4, 8, 6, 10, 12, 14)


def rcopy(src, dst, ss, rs, dev):
    return pltpu.make_async_remote_copy(src_ref=src, dst_ref=dst, send_sem=ss, recv_sem=rs, device_id=(dev,), device_id_type=MESH)


def when(cond, fn):
    pl.when(cond)(fn)


def lanczos_kernel(psi, l_ref, w_ref, r_ref, o_ref, ab_ref,
                   lb, kr, rb, wb, ub, y, zz, acc, got, vb, ps, v0b, fk, tb, rx, ost, sc_out, sc_in, nt_out, nt_in, bp,
                   loc, osem, psem, zs, xys, fws, rsl, rss, rsr, wss, wsr, ns, sw, sss, ssr, uss, usr, ufs, oss, osr, cs):
    me = lax.axis_index("terms")
    c = lax.rem(me, 2)
    s = me // 2
    z = me // 8
    half = me // 16
    m = lax.rem(me, 16)
    b0 = pl.multiple_of(16 * m, 16)
    sib = me ^ 1
    xn, yn = me ^ 2, me ^ 4

    own = [pltpu.make_async_copy(l_ref, lb.at[s, :, pl.ds(0, 384)], loc.at[0]),
           pltpu.make_async_copy(r_ref.at[:, pl.ds(pl.multiple_of(32 * lax.rem(s, 8), 32), 32)], rb.at[s], loc.at[1]),
           pltpu.make_async_copy(w_ref, wb.at[s], loc.at[2]),
           pltpu.make_async_copy(psi.at[:, pl.ds(8 * me, 8)], v0b, loc.at[3])]
    for o in own:
        o.start()

    def p_copy(q):
        return pltpu.make_async_copy(psi.at[half, :, q // 4, lax.rem(q, 4), :], ps.at[lax.rem(q, 4)], psem.at[lax.rem(q, 4)])

    for q in range(4):
        p_copy(q).start()

    bar = pltpu.get_barrier_semaphore()
    for d in range(1, 32):
        pl.semaphore_signal(bar, inc=1, device_id=(me ^ d,), device_id_type=MESH)
    pl.semaphore_wait(bar, 31)

    def lh(src, h):
        return lb.at[src, pl.ds(4 * h, 4), pl.ds(0, 384)]

    def w_copy(d):
        return rcopy(w_ref, wb.at[s], wss.at[d], wsr.at[s], me ^ (2 * d))

    def r_copy(d):
        dst = s ^ d
        return rcopy(r_ref.at[:, pl.ds(pl.multiple_of(32 * lax.rem(dst, 8), 32), 32)], rb.at[s], rss.at[d], rsr.at[s], me ^ (2 * d))

    def z_copy(src, g, h, dev, mine=False):
        return rcopy(l_ref.at[pl.ds(4 * h, 4)] if mine else lh(src, h), lh(src, h), zs.at[g, h], rsl.at[src, h], dev)

    def xy_copies(src, g, mine=False):
        out = []
        for n, (h, dev) in enumerate(((0, xn), (1, yn), (0, yn), (1, xn))):
            out.append(rcopy(l_ref.at[pl.ds(4 * h, 4)] if mine else lh(src, h), lh(src, h), xys.at[g, n], rsl.at[src, h], dev))
        return out

    def f_copy(src, g, h):
        return rcopy(lh(src, h), lh(src, h), fws.at[g, h], rsl.at[src, h], yn if h == 0 else xn)

    def wait_l(src, h):
        rcopy(lh(src, h), lh(src, h), zs.at[0, 0], rsl.at[src, h], xn).wait_recv()

    for d in range(1, 16):
        w_copy(d).start()
    for h in range(2):
        when(z < 3, z_copy(s, 0, h, me + 8, True).start)
        when(z > 0, z_copy(s, 4, h, me - 8, True).start)
    for d in range(1, 8):
        r_copy(d).start()
    for cp in xy_copies(s, 0, True):
        cp.start()

    def square(q, t):
        p_copy(q).wait()
        t = lax.fori_loop(0, 32, lambda n, t: t + ps[lax.rem(q, 4), pl.ds(8 * n, 8), :] * ps[lax.rem(q, 4), pl.ds(8 * n, 8), :], t)
        p_copy(lax.rem(q + 4, 16)).start()
        return t

    total = lax.fori_loop(0, 16, square, jnp.zeros((8, D), F32))
    norm = jnp.sqrt(jnp.sum(total) / N_ELEMS)
    nt_out[...] = jnp.full(TILE, norm, F32)
    ncp = rcopy(nt_out, nt_in, ns.at[0], ns.at[1], me ^ 16)
    ncp.start()

    def first(q, carry):
        p_copy(q).wait()
        t = ps[lax.rem(q, 4)].T / norm
        when(q < 12, lambda: p_copy(q + 4).start())
        acc[0] = t
        ub[q] = t.astype(BF)
        vb[0, pl.ds(pl.multiple_of(16 * q, 16), 16), :] = acc[0, pl.ds(b0, 16), :]
        return carry

    lax.fori_loop(0, 16, first, 0)
    vb[2] = jnp.zeros((D, D), F32)
    bp[...] = jnp.zeros(TILE, F32)
    ab_ref[half] = jnp.zeros(TILE, F32)

    for o in own[:4]:
        o.wait()
    ei = lax.broadcasted_iota(jnp.int32, (D, 16), 0) // 16
    ej = lax.broadcasted_iota(jnp.int32, (D, 16), 1)
    spread = (ei == ej).astype(F32).astype(BF)
    fi = lax.broadcasted_iota(jnp.int32, (H, D), 0)
    fj = lax.broadcasted_iota(jnp.int32, (H, D), 1) // 16
    for k in range(KC):
        fk[k] = (fi == fj + 16 * k).astype(F32).astype(BF)

    def expand(d, carry):
        src = s ^ d
        when(d > 0, lambda: rcopy(w_ref, wb.at[src], wss.at[d], wsr.at[src], me ^ (2 * d)).wait_recv())
        mi = lax.broadcasted_iota(jnp.int32, (D, D), 0) & 15
        mj = lax.broadcasted_iota(jnp.int32, (D, D), 1) & 15
        x = jnp.dot(spread, wb[src], preferred_element_type=F32).astype(BF)
        for k in range(KC):
            e = jnp.dot(x, fk[k], preferred_element_type=F32)
            kr[src, k] = jnp.where(mi == mj, e, 0.0).astype(BF)
        return carry

    lax.fori_loop(0, 16, expand, 0)

    zend = jnp.logical_or(z == 0, z == 3)

    def line(g):
        near = jnp.where(zend, 2, 3)
        step = jnp.where(g == 0, 0, jnp.where(g == 1, 1, jnp.where(g == 2, near, 5 - near)))
        return s ^ (4 * step)

    def arrive(n):
        g, e = n // 4, lax.rem(n, 4)
        base = line(g)
        src = base ^ e

        @pl.when(jnp.logical_and(e == 0, g > 0))
        def _():
            zb = base // 4
            for h in range(2):
                wait_l(base, h)
            up = jnp.logical_and(zb < z, z < 3)
            down = jnp.logical_and(zb > z, z > 0)
            for h in range(2):
                when(up, z_copy(base, g, h, me + 8).start)
                when(down, z_copy(base, g, h, me - 8).start)
            for cp in xy_copies(base, g):
                cp.start()

        @pl.when(n == 4)
        def _():
            for d in range(8, 16):
                r_copy(d).start()

        @pl.when(e == 1)
        def _():
            wait_l(src, 0)
            f_copy(src, g, 0).start()
            wait_l(base ^ 2, 1)
            f_copy(base ^ 2, g, 1).start()
            wait_l(src, 1)

        when(e == 2, lambda: wait_l(src, 0))

        @pl.when(e == 3)
        def _():
            for h in range(2):
                wait_l(src, h)

        when(n > 0, lambda: rcopy(rb.at[src], rb.at[src], rss.at[1], rsr.at[src], xn).wait_recv())
        for k in range(KC):
            lb[src, k, 384:512, :] = lb[src, k, 0:H, :].T

    def right(s0, cnt, u0, y0):
        rr = rb[pl.ds(s0, cnt)].reshape(cnt * KC * 32, D)
        for du in range(4):
            yu = jnp.dot(rr, ub[u0 + du], preferred_element_type=F32).astype(BF).reshape(cnt, KC, 2, 16, D)
            at = pl.ds(pl.multiple_of(16 * (u0 + du), 16), 16)
            for t in range(2):
                y[pl.ds(y0, cnt), :, at, t * D:(t + 1) * D] = yu[:, :, t]

    def chunk(j, n):
        src = line(n // 4) ^ lax.rem(n, 4)
        slot = lax.rem(src, 8)
        when(j == 0, lambda: arrive(n))

        @pl.when(jnp.logical_or(j == 0, n >= 8))
        def _():
            for i in range(4):
                right(src, 1, 4 * i, slot)

        hk = KC // 2
        for h in range(2):
            for k in range(hk):
                zk = jnp.dot(kr[src, hk * h + k], y[slot, hk * h + k], preferred_element_type=F32).astype(BF)
                for t in range(2):
                    zz[t * D:(t + 1) * D, k * D:(k + 1) * D] = zk[:, t * D:(t + 1) * D]
            lk = lb.at[src, hk * h:hk * (h + 1)]
            rhs = jnp.concatenate([lk[:, D:512, :].reshape(hk * D, H), lk[:, 0:D, :].reshape(hk * D, H)], axis=1)
            acc[...] += jnp.dot(zz[...], rhs, preferred_element_type=F32).reshape(2, D, D)

    row = lax.broadcasted_iota(jnp.int32, TILE, 0)
    lane = lax.broadcasted_iota(jnp.int32, TILE, 1)

    def mine(src, g):
        return ub.at[pl.ds(4 * g, 4), pl.ds(pl.multiple_of(16 * src, 16), 16), :]

    def u_copy(d, g):
        return rcopy(mine(m, g), mine(m, g), uss.at[d, g], usr.at[m, g], 16 * half + (m ^ d))

    def u_fwd(d, g):
        return rcopy(mine(m ^ d, g), mine(m ^ d, g), ufs.at[d, g], usr.at[m ^ d, g], sib)

    def u_wait(src, g):
        rcopy(mine(src, g), mine(src, g), uss.at[1, 0], usr.at[src, g], sib).wait_recv()

    def sc_copy(d):
        return rcopy(sc_out, sc_in.at[m], sss.at[d], ssr.at[m], 16 * half + (m ^ d))

    def out_copy(j, p, k):
        return rcopy(tb.at[j, pl.ds(pl.multiple_of(8 * p, 8), 8), :], rx.at[j, me], oss.at[0], osr.at[k], p)

    def step(j, carry):
        @pl.when(j > 0)
        def _():
            def group(g, carry):
                for d in NEAR:
                    u_wait(m ^ d, g)
                    u_fwd(d, g).start()
                for d in range(1, 16, 2):
                    u_wait(m ^ d, g)

                for p in (0, 4):
                    right(8 * half + p, 4, 4 * g, p)
                for d in (1,) + NEAR:
                    u_copy(d, g).wait_send()
                for d in NEAR:
                    u_fwd(d, g).wait_send()
                return carry

            lax.fori_loop(0, 4, group, 0)

        acc[...] = jnp.zeros((2, D, D), F32)

        def chunks(n, carry):
            chunk(j, n)
            return carry

        lax.fori_loop(0, 16, chunks, 0)
        swap = rcopy(acc.at[1 - c], got, sw.at[0], sw.at[1], sib)
        swap.start()
        swap.wait()
        i0, i1, i2 = lax.rem(j, 3), lax.rem(j + 1, 3), lax.rem(j + 2, 3)
        v = vb[i0]
        w = acc[c] + got[...]
        w2 = w - bp[0:1, 0:1] * vb[i2]
        s1 = jnp.sum(w * v)
        s4 = jnp.sum(v * v)
        sh = jnp.sum(w2 * v) / jnp.where(s4 > 0, s4, 1.0)
        w3 = w2 - sh * v
        s2 = jnp.sum(w3 * w3)
        s3 = jnp.sum(w3 * v)
        tile = jnp.zeros(TILE, F32)
        for n, val in enumerate((s1, s2, s3, s4, sh)):
            tile = jnp.where(row == n, val, tile)
        sc_out[...] = tile
        sc_in[m] = tile
        for d in range(1, 16):
            sc_copy(d).start()
        for d in range(1, 16):
            rcopy(sc_out, sc_in.at[m ^ d], sss.at[d], ssr.at[m ^ d], sib).wait_recv()
        alpha = jnp.zeros((1, 1), F32)
        for d in range(16):
            alpha = alpha + sc_in[d, 0:1, 0:1]
        alpha = alpha / N_ELEMS
        beta2 = jnp.zeros((1, 1), F32)
        for d in range(16):
            dl = alpha - sc_in[d, 4:5, 0:1]
            beta2 = beta2 + (sc_in[d, 1:2, 0:1] - 2.0 * dl * sc_in[d, 2:3, 0:1] + dl * dl * sc_in[d, 3:4, 0:1])
        beta = jnp.sqrt(jnp.maximum(beta2, 0.0) / N_ELEMS)
        vn = (w2 - alpha * v) / beta
        more = j < STEPS - 1

        @pl.when(more)
        def _():
            ub[:, pl.ds(b0, 16), :] = vn.astype(BF).reshape(16, 16, D)

        vb[i1] = vn

        @pl.when(more)
        def _():
            for g in range(4):
                for d in (14, 6, 10, 12, 2, 4, 8, 1):
                    u_copy(d, g).start()

        bp[...] = jnp.broadcast_to(beta, TILE)
        ab = jnp.where(row == 0, jnp.broadcast_to(alpha, TILE), jnp.broadcast_to(beta, TILE))
        ab_ref[half] = jnp.where(lane == j, ab, ab_ref[half])
        tb[j] = vb[i1].T
        rx[j, me] = tb[j, pl.ds(pl.multiple_of(8 * me, 8), 8), :]
        k = jnp.where(more, 0, 1)

        @pl.when(jnp.logical_not(more))
        def _():
            for d in range(31, 0, -1):
                out_copy(j, me ^ d, 1).start()

        @pl.when(more)
        def _():
            for d in range(31, 0, -1):
                out_copy(j, me ^ d, 0).start()

        for d in range(1, 16):
            sc_copy(d).wait_send()
        return carry

    lax.fori_loop(0, STEPS, step, 0)

    cross = rcopy(ab_ref.at[half], ab_ref.at[half], cs.at[0], cs.at[1], me ^ 16)
    cross.start()
    ncp.wait()
    for r in range(2):
        v0b[r] = v0b[r] / jnp.where(half == r, norm, nt_in[0:1, 0:1].reshape(1, 1, 1, 1))
        pltpu.make_async_copy(v0b.at[r], o_ref.at[r, 0], osem.at[2 + r]).start()
    grp = lane // 16

    def regroup(n, carry):
        j = n // 2
        r = lax.rem(n, 2)
        when(j > 0, lambda: pltpu.make_async_copy(ost.at[r], o_ref.at[r, j], osem.at[r]).wait())
        for h in range(2):
            for hb in range(2):
                xv = [rx[j, 16 * r + 8 * hb + q, :, h * H:(h + 1) * H] for q in range(8)]
                for d in (1, 2, 4):
                    low = (grp & d) == 0
                    for a in range(8):
                        if a & d == 0:
                            p, q = xv[a], xv[a + d]
                            xv[a] = jnp.where(low, p, pltpu.roll(q, 16 * d, 1))
                            xv[a + d] = jnp.where(low, pltpu.roll(p, H - 16 * d, 1), q)
                for q in range(8):
                    ost[r, :, h * 2 + q // 4, q % 4, hb * H:(hb + 1) * H] = xv[q]
        pltpu.make_async_copy(ost.at[r], o_ref.at[r, j + 1], osem.at[r]).start()
        return carry

    def arrived(lo, cnt, k):
        ref = rx.at[pl.ds(lo, cnt), pl.ds(0, 31)]
        rcopy(ref, ref, oss.at[0], osr.at[k], sib).wait_recv()

    arrived(0, STEPS - 1, 0)
    lax.fori_loop(0, 2 * (STEPS - 1), regroup, 0)
    arrived(STEPS - 1, 1, 1)
    lax.fori_loop(2 * (STEPS - 1), 2 * STEPS, regroup, 0)
    for r in range(2):
        pltpu.make_async_copy(ost.at[r], o_ref.at[r, STEPS], osem.at[r]).wait()
        pltpu.make_async_copy(v0b.at[r], o_ref.at[r, 0], osem.at[2 + r]).wait()
    ref = rx.at[:, pl.ds(0, 31)]
    rcopy(ref, ref, oss.at[0], osr.at[0], sib).wait_send()
    cross.wait()
    for d in range(1, 16):
        w_copy(d).wait_send()
        r_copy(d).wait_send()
    for h in range(2):
        when(z < 3, z_copy(s, 0, h, me + 8, True).wait_send)
        when(z > 0, z_copy(s, 4, h, me - 8, True).wait_send)
    for cp in xy_copies(s, 0, True):
        cp.wait_send()
    for g in range(4):
        base = line(g)
        if g:
            zb = base // 4
            for h in range(2):
                when(jnp.logical_and(zb < z, z < 3), z_copy(base, g, h, me + 8).wait_send)
                when(jnp.logical_and(zb > z, z > 0), z_copy(base, g, h, me - 8).wait_send)
            for cp in xy_copies(base, g):
                cp.wait_send()
        f_copy(base ^ 1, g, 0).wait_send()
        f_copy(base ^ 2, g, 1).wait_send()


def lanczos(psi, l_loc, w_loc, r_loc):
    any_ = pl.BlockSpec(memory_space=pl.ANY)
    vm = pl.BlockSpec(memory_space=VM)
    dma = pltpu.SemaphoreType.DMA
    scratch = [
        VM((16, 8, 512, H), BF), VM((16, 8, D, D), BF), VM((16, 8, 32, D), BF), VM((16, 16, H), BF),
        VM((16, D, D), BF), VM((8, KC, D, 512), BF), VM((512, KC * H), BF), VM((2, D, D), F32), VM((D, D), F32),
        VM((3, D, D), F32), VM((4, D, D), F32), VM((2, 8, 4, 4, D), F32), VM((KC, H, D), BF),
        VM((STEPS, D, D), F32), VM((STEPS, 32, 8, D), F32), VM((2, 8, 4, 4, D), F32),
        VM(TILE, F32), VM((16, 8, H), F32), VM(TILE, F32), VM(TILE, F32), VM(TILE, F32),
        dma((4,)), dma((4,)), dma((4,)), dma((5, 2)), dma((4, 4)), dma((4, 2)), dma((16, 2)), dma((16,)), dma((16,)), dma((16,)), dma((16,)),
        dma((2,)), dma((2,)), dma((16,)), dma((16,)), dma((16, 4)), dma((16, 4)), dma((16, 4)), dma((1,)), dma((2,)), dma((2,)),
    ]
    return pl.pallas_call(
        lanczos_kernel,
        out_shape=(jax.ShapeDtypeStruct((2, STEPS + 1, 8, 4, 4, D), F32), jax.ShapeDtypeStruct((2, 8, H), F32)),
        in_specs=[any_] * 4,
        out_specs=(any_, vm),
        scratch_shapes=scratch,
        compiler_params=pltpu.CompilerParams(collective_id=0, has_side_effects=True, vmem_limit_bytes=63 * 2**20),
    )(psi, l_loc, w_loc, r_loc)


def solution(mesh):
    def device_fn(psi, l_loc, w_loc, r_loc):
        w = w_loc.transpose(2, 0, 1).reshape(16, H)
        l = jnp.concatenate([l_loc[:, :, H:], l_loc[:, :H, :H]], axis=1)
        vecs, ab = lanczos(psi, l, w, r_loc)
        return vecs, ab[:, 0, :STEPS], ab[:, 1, :STEPS]

    return jax.shard_map(device_fn, mesh=mesh, in_specs=(P(), P("terms"), P("terms"), P("terms")),
                         out_specs=(P(None, None, "terms"), P(), P()), check_vma=False)
```

```python
import functools

import jax
import jax.numpy as jnp
from jax import lax
from jax.experimental import pallas as pl
from jax.experimental.pallas import tpu as pltpu
from jax.sharding import PartitionSpec as P

STEPS = 6
KC = 8
BF = jnp.bfloat16
F32 = jnp.float32
MESH = pl.DeviceIdType.MESH
VM = pltpu.VMEM
D, H = 256, 128
N_ELEMS = D * 16 * D
TILE = (8, H)
NEAR = (2, 4, 8, 6, 10, 12, 14)


def rcopy(src, dst, ss, rs, dev):
    return pltpu.make_async_remote_copy(src_ref=src, dst_ref=dst, send_sem=ss, recv_sem=rs, device_id=(dev,), device_id_type=MESH)


def when(cond, fn):
    pl.when(cond)(fn)


def lanczos_kernel(psi, l_ref, w_ref, r_ref, o_ref, ab_ref,
                   lb, kr, rb, wb, ub, y, zz, acc, got, vb, ps, v0b, fk, tb, rx, ost, sc_out, sc_in, nt_out, nt_in, bp,
                   loc, osem, psem, zs, xys, fws, rsl, rss, rsr, wss, wsr, ns, sw, sss, ssr, uss, usr, ufs, oss, osr, cs):
    me = lax.axis_index("terms")
    c = lax.rem(me, 2)
    s = me // 2
    z = me // 8
    half = me // 16
    m = lax.rem(me, 16)
    b0 = pl.multiple_of(16 * m, 16)
    sib = me ^ 1
    xn, yn = me ^ 2, me ^ 4

    own = [pltpu.make_async_copy(l_ref, lb.at[s, :, pl.ds(0, 384)], loc.at[0]),
           pltpu.make_async_copy(r_ref.at[:, pl.ds(pl.multiple_of(32 * lax.rem(s, 8), 32), 32)], rb.at[s], loc.at[1]),
           pltpu.make_async_copy(w_ref, wb.at[s], loc.at[2]),
           pltpu.make_async_copy(psi.at[:, pl.ds(8 * me, 8)], v0b, loc.at[3])]
    for o in own:
        o.start()

    def p_copy(q):
        return pltpu.make_async_copy(psi.at[half, :, q // 4, lax.rem(q, 4), :], ps.at[lax.rem(q, 4)], psem.at[lax.rem(q, 4)])

    for q in range(4):
        p_copy(q).start()

    bar = pltpu.get_barrier_semaphore()
    for d in range(1, 32):
        pl.semaphore_signal(bar, inc=1, device_id=(me ^ d,), device_id_type=MESH)
    pl.semaphore_wait(bar, 31)

    def lh(src, h):
        return lb.at[src, pl.ds(4 * h, 4), pl.ds(0, 384)]

    def w_copy(d):
        return rcopy(w_ref, wb.at[s], wss.at[d], wsr.at[s], me ^ (2 * d))

    def r_copy(d):
        dst = s ^ d
        return rcopy(r_ref.at[:, pl.ds(pl.multiple_of(32 * lax.rem(dst, 8), 32), 32)], rb.at[s], rss.at[d], rsr.at[s], me ^ (2 * d))

    def z_copy(src, g, h, dev, mine=False):
        return rcopy(l_ref.at[pl.ds(4 * h, 4)] if mine else lh(src, h), lh(src, h), zs.at[g, h], rsl.at[src, h], dev)

    def xy_copies(src, g, mine=False):
        out = []
        for n, (h, dev) in enumerate(((0, xn), (1, yn), (0, yn), (1, xn))):
            out.append(rcopy(l_ref.at[pl.ds(4 * h, 4)] if mine else lh(src, h), lh(src, h), xys.at[g, n], rsl.at[src, h], dev))
        return out

    def f_copy(src, g, h):
        return rcopy(lh(src, h), lh(src, h), fws.at[g, h], rsl.at[src, h], yn if h == 0 else xn)

    def wait_l(src, h):
        rcopy(lh(src, h), lh(src, h), zs.at[0, 0], rsl.at[src, h], xn).wait_recv()

    for d in range(1, 16):
        w_copy(d).start()
    for h in range(2):
        when(z < 3, z_copy(s, 0, h, me + 8, True).start)
        when(z > 0, z_copy(s, 4, h, me - 8, True).start)
    for d in (1, 2, 3, 4, 8, 5, 6, 7) + tuple(range(9, 16)):
        r_copy(d).start()
    for cp in xy_copies(s, 0, True):
        cp.start()

    def square(q, t):
        p_copy(q).wait()
        t = lax.fori_loop(0, 32, lambda n, t: t + ps[lax.rem(q, 4), pl.ds(8 * n, 8), :] * ps[lax.rem(q, 4), pl.ds(8 * n, 8), :], t)
        p_copy(lax.rem(q + 4, 16)).start()
        return t

    total = lax.fori_loop(0, 16, square, jnp.zeros((8, D), F32))
    norm = jnp.sqrt(jnp.sum(total) / N_ELEMS)
    nt_out[...] = jnp.full(TILE, norm, F32)
    ncp = rcopy(nt_out, nt_in, ns.at[0], ns.at[1], me ^ 16)
    ncp.start()

    def first(q, carry):
        p_copy(q).wait()
        t = ps[lax.rem(q, 4)].T / norm
        when(q < 12, lambda: p_copy(q + 4).start())
        acc[0] = t
        ub[q] = t.astype(BF)
        vb[0, pl.ds(pl.multiple_of(16 * q, 16), 16), :] = acc[0, pl.ds(b0, 16), :]
        return carry

    lax.fori_loop(0, 16, first, 0)
    vb[2] = jnp.zeros((D, D), F32)
    bp[...] = jnp.zeros(TILE, F32)
    ab_ref[half] = jnp.zeros(TILE, F32)

    for o in own[:4]:
        o.wait()
    ei = lax.broadcasted_iota(jnp.int32, (D, 16), 0) // 16
    ej = lax.broadcasted_iota(jnp.int32, (D, 16), 1)
    spread = (ei == ej).astype(F32).astype(BF)
    fi = lax.broadcasted_iota(jnp.int32, (H, D), 0)
    fj = lax.broadcasted_iota(jnp.int32, (H, D), 1) // 16
    for k in range(KC):
        fk[k] = (fi == fj + 16 * k).astype(F32).astype(BF)

    def expand(d, carry):
        src = s ^ d
        when(d > 0, lambda: rcopy(w_ref, wb.at[src], wss.at[d], wsr.at[src], me ^ (2 * d)).wait_recv())
        mi = lax.broadcasted_iota(jnp.int32, (D, D), 0) & 15
        mj = lax.broadcasted_iota(jnp.int32, (D, D), 1) & 15
        x = jnp.dot(spread, wb[src], preferred_element_type=F32).astype(BF)
        for k in range(KC):
            e = jnp.dot(x, fk[k], preferred_element_type=F32)
            kr[src, k] = jnp.where(mi == mj, e, 0.0).astype(BF)
        return carry

    lax.fori_loop(0, 16, expand, 0)

    zend = jnp.logical_or(z == 0, z == 3)

    def line(g):
        near = jnp.where(zend, 2, 3)
        step = jnp.where(g == 0, 0, jnp.where(g == 1, 1, jnp.where(g == 2, near, 5 - near)))
        return s ^ (4 * step)

    def arrive(n):
        g, e = n // 4, lax.rem(n, 4)
        base = line(g)
        src = base ^ e

        @pl.when(jnp.logical_and(e == 0, g > 0))
        def _():
            zb = base // 4
            for h in range(2):
                wait_l(base, h)
            up = jnp.logical_and(zb < z, z < 3)
            down = jnp.logical_and(zb > z, z > 0)
            for h in range(2):
                when(up, z_copy(base, g, h, me + 8).start)
                when(down, z_copy(base, g, h, me - 8).start)
            for cp in xy_copies(base, g):
                cp.start()

        @pl.when(e == 1)
        def _():
            wait_l(src, 0)
            f_copy(src, g, 0).start()
            wait_l(base ^ 2, 1)
            f_copy(base ^ 2, g, 1).start()
            wait_l(src, 1)

        when(e == 2, lambda: wait_l(src, 0))

        @pl.when(e == 3)
        def _():
            for h in range(2):
                wait_l(src, h)

        when(n > 0, lambda: rcopy(rb.at[src], rb.at[src], rss.at[1], rsr.at[src], xn).wait_recv())
        for k in range(KC):
            lb[src, k, 384:512, :] = lb[src, k, 0:H, :].T

    def right(s0, cnt, u0, y0):
        rr = rb[pl.ds(s0, cnt)].reshape(cnt * KC * 32, D)
        for du in range(4):
            yu = jnp.dot(rr, ub[u0 + du], preferred_element_type=F32).astype(BF).reshape(cnt, KC, 2, 16, D)
            at = pl.ds(pl.multiple_of(16 * (u0 + du), 16), 16)
            for t in range(2):
                y[pl.ds(y0, cnt), :, at, t * D:(t + 1) * D] = yu[:, :, t]

    def chunk(j, n):
        src = line(n // 4) ^ lax.rem(n, 4)
        slot = lax.rem(src, 8)
        when(j == 0, lambda: arrive(n))

        @pl.when(jnp.logical_or(j == 0, n >= 8))
        def _():
            for i in range(4):
                right(src, 1, 4 * i, slot)

        hk = KC // 2
        for h in range(2):
            for k in range(hk):
                zk = jnp.dot(kr[src, hk * h + k], y[slot, hk * h + k], preferred_element_type=F32).astype(BF)
                for t in range(2):
                    zz[t * D:(t + 1) * D, k * D:(k + 1) * D] = zk[:, t * D:(t + 1) * D]
            lk = lb.at[src, hk * h:hk * (h + 1)]
            rhs = jnp.concatenate([lk[:, D:512, :].reshape(hk * D, H), lk[:, 0:D, :].reshape(hk * D, H)], axis=1)
            acc[...] += jnp.dot(zz[...], rhs, preferred_element_type=F32).reshape(2, D, D)

    row = lax.broadcasted_iota(jnp.int32, TILE, 0)
    lane = lax.broadcasted_iota(jnp.int32, TILE, 1)

    def mine(src, g):
        return ub.at[pl.ds(4 * g, 4), pl.ds(pl.multiple_of(16 * src, 16), 16), :]

    def u_copy(d, g):
        return rcopy(mine(m, g), mine(m, g), uss.at[d, g], usr.at[m, g], 16 * half + (m ^ d))

    def u_fwd(d, g):
        return rcopy(mine(m ^ d, g), mine(m ^ d, g), ufs.at[d, g], usr.at[m ^ d, g], sib)

    def u_wait(src, g):
        rcopy(mine(src, g), mine(src, g), uss.at[1, 0], usr.at[src, g], sib).wait_recv()

    def sc_copy(d):
        return rcopy(sc_out, sc_in.at[m], sss.at[d], ssr.at[m], 16 * half + (m ^ d))

    def out_copy(j, p, k):
        return rcopy(tb.at[j, pl.ds(pl.multiple_of(8 * p, 8), 8), :], rx.at[j, me], oss.at[0], osr.at[k], p)

    def step(j, carry):
        @pl.when(j > 0)
        def _():
            def group(g, carry):
                for d in NEAR:
                    u_wait(m ^ d, g)
                    u_fwd(d, g).start()
                for d in range(1, 16, 2):
                    u_wait(m ^ d, g)

                for p in (0, 4):
                    right(8 * half + p, 4, 4 * g, p)
                for d in (1,) + NEAR:
                    u_copy(d, g).wait_send()
                for d in NEAR:
                    u_fwd(d, g).wait_send()
                return carry

            lax.fori_loop(0, 4, group, 0)
            for d in range(31, 0, -1):
                out_copy(j - 1, me ^ d, 0).start()

        acc[...] = jnp.zeros((2, D, D), F32)

        def chunks(n, carry):
            chunk(j, n)
            return carry

        lax.fori_loop(0, 16, chunks, 0)
        swap = rcopy(acc.at[1 - c], got, sw.at[0], sw.at[1], sib)
        swap.start()
        swap.wait()
        i0, i1, i2 = lax.rem(j, 3), lax.rem(j + 1, 3), lax.rem(j + 2, 3)
        v = vb[i0]
        w = acc[c] + got[...]
        w2 = w - bp[0:1, 0:1] * vb[i2]
        s1 = jnp.sum(w * v)
        s4 = jnp.sum(v * v)
        sh = jnp.sum(w2 * v) / jnp.where(s4 > 0, s4, 1.0)
        w3 = w2 - sh * v
        s2 = jnp.sum(w3 * w3)
        s3 = jnp.sum(w3 * v)
        tile = jnp.zeros(TILE, F32)
        for n, val in enumerate((s1, s2, s3, s4, sh)):
            tile = jnp.where(row == n, val, tile)
        sc_out[...] = tile
        sc_in[m] = tile
        for d in range(1, 16):
            sc_copy(d).start()
        for d in range(1, 16):
            rcopy(sc_out, sc_in.at[m ^ d], sss.at[d], ssr.at[m ^ d], sib).wait_recv()
        alpha = jnp.zeros((1, 1), F32)
        for d in range(16):
            alpha = alpha + sc_in[d, 0:1, 0:1]
        alpha = alpha / N_ELEMS
        beta2 = jnp.zeros((1, 1), F32)
        for d in range(16):
            dl = alpha - sc_in[d, 4:5, 0:1]
            beta2 = beta2 + (sc_in[d, 1:2, 0:1] - 2.0 * dl * sc_in[d, 2:3, 0:1] + dl * dl * sc_in[d, 3:4, 0:1])
        beta = jnp.sqrt(jnp.maximum(beta2, 0.0) / N_ELEMS)
        vn = (w2 - alpha * v) / beta
        more = j < STEPS - 1

        @pl.when(more)
        def _():
            ub[:, pl.ds(b0, 16), :] = vn.astype(BF).reshape(16, 16, D)

        vb[i1] = vn

        @pl.when(more)
        def _():
            for g in range(4):
                for d in (14, 6, 10, 12, 2, 4, 8, 1):
                    u_copy(d, g).start()

        bp[...] = jnp.broadcast_to(beta, TILE)
        ab = jnp.where(row == 0, jnp.broadcast_to(alpha, TILE), jnp.broadcast_to(beta, TILE))
        ab_ref[half] = jnp.where(lane == j, ab, ab_ref[half])
        tb[j] = vb[i1].T
        rx[j, me] = tb[j, pl.ds(pl.multiple_of(8 * me, 8), 8), :]

        @pl.when(jnp.logical_not(more))
        def _():
            for d in range(31, 0, -1):
                out_copy(j, me ^ d, 1).start()

        for d in range(1, 16):
            sc_copy(d).wait_send()
        return carry

    lax.fori_loop(0, STEPS, step, 0)

    cross = rcopy(ab_ref.at[half], ab_ref.at[half], cs.at[0], cs.at[1], me ^ 16)
    cross.start()
    ncp.wait()
    for r in range(2):
        v0b[r] = v0b[r] / jnp.where(half == r, norm, nt_in[0:1, 0:1].reshape(1, 1, 1, 1))
        pltpu.make_async_copy(v0b.at[r], o_ref.at[r, 0], osem.at[2 + r]).start()
    grp = lane // 16

    def regroup(n, carry):
        j = n // 2
        r = lax.rem(n, 2)
        when(j > 0, lambda: pltpu.make_async_copy(ost.at[r], o_ref.at[r, j], osem.at[r]).wait())
        for h in range(2):
            for hb in range(2):
                xv = [rx[j, 16 * r + 8 * hb + q, :, h * H:(h + 1) * H] for q in range(8)]
                for d in (1, 2, 4):
                    low = (grp & d) == 0
                    for a in range(8):
                        if a & d == 0:
                            p, q = xv[a], xv[a + d]
                            xv[a] = jnp.where(low, p, pltpu.roll(q, 16 * d, 1))
                            xv[a + d] = jnp.where(low, pltpu.roll(p, H - 16 * d, 1), q)
                for q in range(8):
                    ost[r, :, h * 2 + q // 4, q % 4, hb * H:(hb + 1) * H] = xv[q]
        pltpu.make_async_copy(ost.at[r], o_ref.at[r, j + 1], osem.at[r]).start()
        return carry

    def arrived(lo, cnt, k):
        ref = rx.at[pl.ds(lo, cnt), pl.ds(0, 31)]
        rcopy(ref, ref, oss.at[0], osr.at[k], sib).wait_recv()

    arrived(0, STEPS - 1, 0)
    lax.fori_loop(0, 2 * (STEPS - 1), regroup, 0)
    arrived(STEPS - 1, 1, 1)
    lax.fori_loop(2 * (STEPS - 1), 2 * STEPS, regroup, 0)
    for r in range(2):
        pltpu.make_async_copy(ost.at[r], o_ref.at[r, STEPS], osem.at[r]).wait()
        pltpu.make_async_copy(v0b.at[r], o_ref.at[r, 0], osem.at[2 + r]).wait()
    ref = rx.at[:, pl.ds(0, 31)]
    rcopy(ref, ref, oss.at[0], osr.at[0], sib).wait_send()
    cross.wait()
    for d in range(1, 16):
        w_copy(d).wait_send()
        r_copy(d).wait_send()
    for h in range(2):
        when(z < 3, z_copy(s, 0, h, me + 8, True).wait_send)
        when(z > 0, z_copy(s, 4, h, me - 8, True).wait_send)
    for cp in xy_copies(s, 0, True):
        cp.wait_send()
    for g in range(4):
        base = line(g)
        if g:
            zb = base // 4
            for h in range(2):
                when(jnp.logical_and(zb < z, z < 3), z_copy(base, g, h, me + 8).wait_send)
                when(jnp.logical_and(zb > z, z > 0), z_copy(base, g, h, me - 8).wait_send)
            for cp in xy_copies(base, g):
                cp.wait_send()
        f_copy(base ^ 1, g, 0).wait_send()
        f_copy(base ^ 2, g, 1).wait_send()


def lanczos(psi, l_loc, w_loc, r_loc):
    any_ = pl.BlockSpec(memory_space=pl.ANY)
    vm = pl.BlockSpec(memory_space=VM)
    dma = pltpu.SemaphoreType.DMA
    scratch = [
        VM((16, 8, 512, H), BF), VM((16, 8, D, D), BF), VM((16, 8, 32, D), BF), VM((16, 16, H), BF),
        VM((16, D, D), BF), VM((8, KC, D, 512), BF), VM((512, KC * H), BF), VM((2, D, D), F32), VM((D, D), F32),
        VM((3, D, D), F32), VM((4, D, D), F32), VM((2, 8, 4, 4, D), F32), VM((KC, H, D), BF),
        VM((STEPS, D, D), F32), VM((STEPS, 32, 8, D), F32), VM((2, 8, 4, 4, D), F32),
        VM(TILE, F32), VM((16, 8, H), F32), VM(TILE, F32), VM(TILE, F32), VM(TILE, F32),
        dma((4,)), dma((4,)), dma((4,)), dma((5, 2)), dma((4, 4)), dma((4, 2)), dma((16, 2)), dma((16,)), dma((16,)), dma((16,)), dma((16,)),
        dma((2,)), dma((2,)), dma((16,)), dma((16,)), dma((16, 4)), dma((16, 4)), dma((16, 4)), dma((1,)), dma((2,)), dma((2,)),
    ]
    return pl.pallas_call(
        lanczos_kernel,
        out_shape=(jax.ShapeDtypeStruct((2, STEPS + 1, 8, 4, 4, D), F32), jax.ShapeDtypeStruct((2, 8, H), F32)),
        in_specs=[any_] * 4,
        out_specs=(any_, vm),
        scratch_shapes=scratch,
        compiler_params=pltpu.CompilerParams(collective_id=0, has_side_effects=True, vmem_limit_bytes=63 * 2**20),
    )(psi, l_loc, w_loc, r_loc)


def solution(mesh):
    def device_fn(psi, l_loc, w_loc, r_loc):
        w = w_loc.transpose(2, 0, 1).reshape(16, H)
        l = jnp.concatenate([l_loc[:, :, H:], l_loc[:, :H, :H]], axis=1)
        vecs, ab = lanczos(psi, l, w, r_loc)
        return vecs, ab[:, 0, :STEPS], ab[:, 1, :STEPS]

    return jax.shard_map(device_fn, mesh=mesh, in_specs=(P(), P("terms"), P("terms"), P("terms")),
                         out_specs=(P(None, None, "terms"), P(), P()), check_vma=False)
```
